32 devices in a mesh: row: 4 (over y, x), col: 8 (over z, core).
Axes of the slice: x: 2, y: 2, z: 4, core: 2. Of those that a mesh axis runs over, the one named last changes fastest.
Arguments:
- voltages: bfloat16 [4096, 32, 2, 256], P(('col', 'row')), may hold values from -6 to 6
- auto_prev: float32 [32, 4096], P('row', 'col'), may hold values from 0.5 to 8
- station_order: int32 [4096], replicated, may hold values from 0 to 4095, each once
Outputs:
- visibilities: bfloat16 [32, 5, 4096, 1024], P('row', None, 'col')
The draws below stay inside these ranges and needn't reach their ends.
Inputs may be any that keep to these rules, and one draw needn't show every extreme that they name: `station_order`: a permutation of the block positions.
All inputs are finite; a program needn't handle non-finite values.
Results may differ from the reference program's by a relative error of at most 0.001.
Values may be sent and summed in bfloat16 or wider, within the bound.
No kernel may reach another device: no remote copies, remote signals or barrier semaphores. Data moves between devices by JAX's collectives and lax.ppermute only.
A program may use at most 192 MiB of HBM per device.

```python
import math
import jax
import jax.numpy as jnp
from jax import lax

STATIONS = 4096
SAMPLES = 256
CHANNELS = 32
N_COL = 8


def level_of(own_key, dims, cuts, least, top_value):
    loudness, own = 1.0, jax.random.fold_in(own_key, 6)
    for axis_at, parts in cuts:
        steps = jnp.exp(jax.random.uniform(jax.random.fold_in(own, axis_at), (parts,), jnp.float32, least / len(cuts), top_value / len(cuts)))
        loudness = loudness * jnp.repeat(steps, dims[axis_at] // parts).reshape([-1 if axis == axis_at else 1 for axis in range(len(dims))])
    return loudness


def gaussian(stream_key, dims, width, bound, cuts=(), held_as=jnp.bfloat16):
    result = jax.random.normal(stream_key, dims, jnp.float32) * width
    if len(cuts) > 0:
        result = level_of(stream_key, dims, cuts, -0.22, 0.18) * result
    return jnp.clip(result, min=-bound, max=bound).astype(held_as)


def setup_inputs(seed: int = 0) -> dict:
    splits = jax.random.split(jax.random.key(seed), 4)
    voltages = gaussian(splits[0], (STATIONS, CHANNELS, 2, SAMPLES), 1.0, 6.0, ((0, 32),))
    auto_prev = jnp.clip(jnp.exp(math.log(8.0) - 2.7725887 * jax.random.uniform(splits[1], (CHANNELS, STATIONS), jnp.float32) ** level_of(splits[1], (CHANNELS, STATIONS), ((0, 4), (1, 8)), -0.2, 0.2)), 0.5, 8.0)
    station_order = jax.random.permutation(splits[2], STATIONS).astype(jnp.int32)
    return {"voltages": voltages, "auto_prev": auto_prev, "station_order": station_order}


def reference(voltages, auto_prev, station_order):
    block_size = STATIONS // N_COL
    offsets = N_COL // 2 + 1
    flat = voltages.reshape(STATIONS, CHANNELS, 2 * SAMPLES)
    turned = jnp.concatenate([-voltages[:, :, 1], voltages[:, :, 0]], axis=-1)
    inverse = 1.0 / jnp.sqrt(auto_prev[:, station_order])

    def one_block(block_index):
        first = (block_index * block_size).astype(jnp.int32)
        own_rows = lax.dynamic_slice_in_dim(flat, first, block_size, 0).astype(jnp.float32)
        row_scale = lax.dynamic_slice_in_dim(inverse, first, block_size, 1)
        tiles = []
        for offset in range(offsets):
            start = ((block_index - offset) % N_COL * block_size).astype(jnp.int32)
            partner = jnp.concatenate([lax.dynamic_slice_in_dim(flat, start, block_size, 0), lax.dynamic_slice_in_dim(turned, start, block_size, 0)], axis=0).astype(jnp.float32)
            gram = jnp.einsum('ich,jch->cij', own_rows, partner)
            column_scale = lax.dynamic_slice_in_dim(inverse, start, block_size, 1)
            column_scale = jnp.concatenate([column_scale, column_scale], axis=-1)
            tiles.append(gram * row_scale[:, :, None] * column_scale[:, None, :] * (1.0 / SAMPLES))
        return jnp.stack(tiles, axis=1).astype(jnp.bfloat16)
    blocks = lax.map(one_block, jnp.arange(N_COL, dtype=jnp.int32))
    blocks = jnp.transpose(blocks, (1, 2, 0, 3, 4))
    return blocks.reshape(CHANNELS, offsets, STATIONS, 2 * block_size)
```

```python
import jax
import jax.numpy as jnp
from jax import lax
from jax.experimental import pallas as pl
from jax.experimental.pallas import tpu as pltpu
from jax.sharding import PartitionSpec as P

LANES = 128


def swap_with(value, axis, distance):
    count = lax.axis_size(axis)
    return lax.ppermute(value, axis, [(i, i ^ distance) for i in range(count)])


def from_behind(value, axis):
    count = lax.axis_size(axis)
    return lax.ppermute(value, axis, [(i, (i + 1) % count) for i in range(count)])


def turned_of(rows):
    half = rows.shape[-1] // 2
    return jnp.concatenate([-rows[:, half:], rows[:, :half]], axis=-1)


def gram_of(left, right):
    return lax.dot_general(
        left, right, (((1,), (1,)), ((), ())), preferred_element_type=jnp.float32
    )


def store_rows(out_ref, gram, where_ref, row_scale_ref, column_scale, first_column, count):
    height, width = gram.shape[0] // count, gram.shape[1]
    for piece in range(count):
        top = pl.multiple_of(where_ref[1 + piece] * height, height)
        row_scale = row_scale_ref[0, pl.ds(top, height), :]
        for lane in range(0, width, LANES):
            part = gram[piece * height : (piece + 1) * height, lane : lane + LANES]
            scaled = part * row_scale * column_scale[:, lane : lane + LANES]
            column = first_column + lane
            if not isinstance(column, int):
                column = pl.multiple_of(column, LANES)
            out_ref[0, 0, pl.ds(top, height), pl.ds(column, LANES)] = scaled.astype(out_ref.dtype)


def whole_tile(count, where_ref, *refs):
    own, partner = refs[:count], refs[count : 2 * count]
    row_scale_ref, column_scale_ref = refs[2 * count : 2 * count + 2]
    out_ref = refs[-1]
    left = jnp.concatenate([ref[0] for ref in own], axis=0)
    for piece in range(count):
        right = partner[piece][0]
        width = right.shape[0]
        first = where_ref[1 + piece] * width
        first = pl.multiple_of(first, LANES)
        scale = column_scale_ref[0, :, pl.ds(first, width)]
        gram = gram_of(left, jnp.concatenate([right, turned_of(right)], axis=0))
        store_rows(out_ref, gram[:, :width], where_ref, row_scale_ref, scale, first, count)
        store_rows(
            out_ref, gram[:, width:], where_ref, row_scale_ref, scale, count * width + first, count
        )


def one_piece(count, where_ref, *refs):
    own, partner = refs[:count], refs[count]
    row_scale_ref, column_scale_ref = refs[count + 1 : count + 3]
    out_ref = refs[-1]
    left = jnp.concatenate([ref[0] for ref in own], axis=0)
    right = partner[0]
    right = jnp.where(pl.program_id(1) == 0, right, turned_of(right))
    scale = column_scale_ref[0]
    store_rows(out_ref, gram_of(left, right), where_ref, row_scale_ref, scale, 0, count)


def tile_call(out, shape, where, own, partner, row_scale, column_scale, offset, piece=None):
    chan_count, _, block_size, _ = shape
    count, (_, height, depth) = len(own), own[0].shape
    rows_spec = pl.BlockSpec((1, height, depth), lambda c, *_: (c, 0, 0))
    row_scale_spec = pl.BlockSpec((1, block_size, LANES), lambda c, *_: (c, 0, 0))
    if piece is None:
        grid = (chan_count,)
        body = lambda *refs: whole_tile(count, *refs)
        column_spec = pl.BlockSpec((1, 1, block_size), lambda c, at: (c, 0, at[0]))
        out_spec = pl.BlockSpec((1, 1, block_size, 2 * block_size), lambda c, at: (c, offset, 0, 0))
        partners = list(partner)
        width = 2 * block_size
    else:
        grid = (chan_count, 2)
        body = lambda *refs: one_piece(count, *refs)
        column_spec = pl.BlockSpec(
            (1, 1, height), lambda c, h, at: (c, 0, at[0] * count + at[1 + piece])
        )
        out_spec = pl.BlockSpec(
            (1, 1, block_size, height), lambda c, h, at: (c, offset, 0, h * count + at[1 + piece])
        )
        partners = [partner[piece]]
        width = 2 * height
    operands = [*own, *partners, row_scale, column_scale]
    in_specs = [rows_spec] * (count + len(partners)) + [row_scale_spec, column_spec]
    aliases = {}
    if out is not None:
        aliases = {1 + len(operands): 0}
        operands.append(out)
        in_specs.append(pl.BlockSpec(memory_space=pl.ANY))
    return pl.pallas_call(
        body,
        grid_spec=pltpu.PrefetchScalarGridSpec(
            num_scalar_prefetch=1, grid=grid, in_specs=in_specs, out_specs=out_spec
        ),
        out_shape=jax.ShapeDtypeStruct(shape, jnp.bfloat16),
        input_output_aliases=aliases,
        cost_estimate=pl.CostEstimate(
            flops=2 * chan_count * block_size * width * depth,
            bytes_accessed=2 * chan_count * block_size * (width + 2 * depth),
            transcendentals=0,
        ),
    )(where, *operands)


def per_device(voltages, auto_prev, station_order):
    rows, cols = lax.axis_size("row"), lax.axis_size("col")
    row, col = lax.axis_index("row"), lax.axis_index("col")
    height, all_channels, parts, samples = voltages.shape
    chan_count = all_channels // rows
    block_size = height * rows
    offsets = cols // 2 + 1

    def piece_for(distance):
        chosen = lax.dynamic_slice_in_dim(voltages, (row ^ distance) * chan_count, chan_count, 1)
        chosen = chosen.reshape(height, chan_count, parts * samples)
        return jnp.transpose(chosen, (1, 0, 2))

    own = [piece_for(0)]
    for distance in range(1, rows):
        own.append(swap_with(piece_for(distance), "row", distance))
    places = [(row ^ distance).astype(jnp.int32) for distance in range(rows)]
    if height % LANES != 0:
        stacked = jnp.take(jnp.stack(own, axis=1), jnp.stack(places), axis=1)
        own = [stacked.reshape(chan_count, block_size, parts * samples)]
        places = [jnp.zeros((), jnp.int32)]
    partners = [own]
    for _ in range(1, offsets):
        partners.append([from_behind(piece, "col") for piece in partners[-1]])

    autos = auto_prev
    distance = 1
    while distance < cols:
        autos = jnp.concatenate([autos, swap_with(autos, "col", distance)], axis=1)
        distance *= 2
    slot = (station_order // block_size) ^ col
    chosen = jnp.take(autos, slot * block_size + station_order % block_size, axis=1)
    inverse = 1.0 / jnp.sqrt(chosen)
    row_scale = lax.dynamic_slice_in_dim(inverse, col * block_size, block_size, 1)
    row_scale = jnp.broadcast_to(
        (row_scale * (1.0 / samples))[:, :, None], (chan_count, block_size, LANES)
    )
    column_scale = inverse[:, None, :]

    shape = (chan_count, offsets, block_size, 2 * block_size)
    out = None
    for offset in range(offsets):
        where = jnp.stack([((col - offset) % cols).astype(jnp.int32), *places])
        pieces = [None] if offset < offsets - 1 or len(own) == 1 else range(len(own))
        for piece in pieces:
            out = tile_call(
                out, shape, where, own, partners[offset], row_scale, column_scale, offset, piece
            )
    return out


def solution(mesh):
    return jax.shard_map(
        per_device,
        mesh=mesh,
        in_specs=(P(("col", "row"), None, None, None), P("row", "col"), P()),
        out_specs=P("row", None, "col", None),
        check_vma=False,
    )
```

```python
import jax
import jax.numpy as jnp
from jax import lax
from jax.experimental import pallas as pl
from jax.experimental.pallas import tpu as pltpu
from jax.sharding import PartitionSpec as P


LANES = 128
VMEM_LIMIT = 253 * 256 * 1024


def swap_with(value, axis, distance):
    count = lax.axis_size(axis)
    return lax.ppermute(value, axis, [(i, i ^ distance) for i in range(count)])


def from_behind(value, axis):
    count = lax.axis_size(axis)
    return lax.ppermute(value, axis, [(i, (i + 1) % count) for i in range(count)])


def rows_distance(turn, parity, rows):
    if parity == 1 and turn in (1, 2) and rows > 2:
        return 3 - turn
    return turn


def traded(value, turn):
    rows, cols = lax.axis_size("row"), lax.axis_size("col")
    pairs = []
    for row in range(rows):
        for col in range(cols):
            other = row ^ rows_distance(turn, col % 2, rows)
            pairs.append((row * cols + col, other * cols + col))
    return lax.ppermute(value, ("row", "col"), pairs)


def gather_piece(group_ref, voltages_ref, out_ref):
    stations, chan_count, parts, samples = voltages_ref.shape
    for chan in range(chan_count):
        out_ref[chan] = voltages_ref[:, chan, :, :].reshape(stations, parts * samples)


def piece_of(voltages, group, chan_count):
    stations, _, parts, samples = voltages.shape
    steps = 2 if stations % 32 == 0 else 1
    some = stations // steps
    return pl.pallas_call(
        gather_piece,
        grid_spec=pltpu.PrefetchScalarGridSpec(
            num_scalar_prefetch=1,
            grid=(steps,),
            in_specs=[
                pl.BlockSpec((some, chan_count, parts, samples), lambda i, at: (i, at[0], 0, 0))
            ],
            out_specs=pl.BlockSpec((chan_count, some, parts * samples), lambda i, at: (0, i, 0)),
        ),
        out_shape=jax.ShapeDtypeStruct((chan_count, stations, parts * samples), voltages.dtype),
    )(group, voltages)


def turned_of(rows):
    half = rows.shape[-1] // 2
    return jnp.concatenate([-rows[:, half:], rows[:, :half]], axis=-1)


def gram_of(left, right):
    return lax.dot_general(
        left, right, (((1,), (1,)), ((), ())), preferred_element_type=jnp.float32
    )


def tiles_kernel(count, chosen, offset, column_start, slots, places_ref, *refs):
    own, partner = refs[:count], refs[count : count + len(chosen)]
    row_scale_ref, column_scale_ref = refs[count + len(chosen) : count + len(chosen) + 2]
    out_ref, left_ref, right_ref, rows_ref, columns_ref, stage_ref, loaded, read, sent = refs[-9:]
    chan_count, height, _ = own[0].shape
    block_size = height * count
    whole = len(chosen) == count
    width = height * len(chosen)
    first_column = column_start
    if not whole:
        first_column = pl.multiple_of(column_start + places_ref[count + chosen[0]] * height, LANES)

    def loads(chan):
        result = []
        for index, ref in enumerate([*own, *partner]):
            to_ref = left_ref if index < count else right_ref
            top = 0
            if index < count or whole:
                top = pl.multiple_of(places_ref[index] * height, height)
            result.append((ref.at[chan], to_ref.at[chan, pl.ds(top, height)]))
        result.append((row_scale_ref.at[chan], rows_ref.at[chan]))
        return [
            pltpu.make_async_copy(source, target, loaded.at[chan, index])
            for index, (source, target) in enumerate(result)
        ]

    def sends(chan):
        slot = chan % slots
        if whole:
            return [pltpu.make_async_copy(stage_ref.at[slot], out_ref.at[chan, offset], sent.at[slot, 0])]
        result = []
        for part in range(2):
            column = part * block_size + places_ref[count + chosen[0]] * height
            column = pl.multiple_of(column, LANES)
            result.append(
                pltpu.make_async_copy(
                    stage_ref.at[slot, :, pl.ds(part * height, height)],
                    out_ref.at[chan, offset, :, pl.ds(column, height)],
                    sent.at[slot, part],
                )
            )
        return result

    columns_load = pltpu.make_async_copy(
        column_scale_ref.at[:, :, pl.ds(first_column, width)], columns_ref, read
    )
    columns_load.start()

    def start_loads(chan, carry):
        for copy in loads(chan):
            copy.start()
        return carry

    lax.fori_loop(0, chan_count, start_loads, 0)
    columns_load.wait()

    def one_channel(chan, carry):
        slot = chan % slots
        for copy in loads(chan):
            copy.wait()
        if slots < chan_count:

            @pl.when(chan >= slots)
            def _():
                for copy in sends(chan - slots):
                    copy.wait()

        left = left_ref[chan]
        row_scale = rows_ref[chan]
        for lane in range(0, width, LANES):
            right = right_ref[chan, lane : lane + LANES, :]
            gram = gram_of(left, jnp.concatenate([right, turned_of(right)], axis=0))
            scale = columns_ref[chan, :, lane : lane + LANES]
            for part in range(2):
                tile = gram[:, part * LANES : (part + 1) * LANES] * row_scale * scale
                column = part * width + lane
                stage_ref[slot, :, column : column + LANES] = tile.astype(stage_ref.dtype)
        for copy in sends(chan):
            copy.start()
        return carry

    lax.fori_loop(0, chan_count, one_channel, 0)

    def drain(chan, carry):
        for copy in sends(chan):
            copy.wait()
        return carry

    lax.fori_loop(chan_count - slots, chan_count, drain, 0)


def tile_call(out, shape, places, own, partner, row_scale, column_scale, offset, chosen):
    chan_count, offsets, block_size, _ = shape
    count, (_, height, depth) = len(own), own[0].shape
    slots = 2 if len(chosen) == count else chan_count
    width = height * len(chosen)
    operands = [*own, *[partner[piece] for piece in chosen], row_scale, column_scale]
    aliases = {}
    if out is not None:
        aliases = {1 + len(operands): 0}
        operands.append(out)
    in_specs = [pl.BlockSpec(memory_space=pltpu.SMEM)]
    in_specs += [pl.BlockSpec(memory_space=pl.ANY)] * len(operands)
    column_start = (offsets - 1 - offset) * block_size

    def body(*refs):
        tiles_kernel(count, chosen, offset, column_start, slots, *refs)

    return pl.pallas_call(
        body,
        in_specs=in_specs,
        out_specs=pl.BlockSpec(memory_space=pl.ANY),
        out_shape=jax.ShapeDtypeStruct(shape, jnp.bfloat16),
        scratch_shapes=[
            pltpu.VMEM((chan_count, block_size, depth), jnp.bfloat16),
            pltpu.VMEM((chan_count, width, depth), jnp.bfloat16),
            pltpu.VMEM((chan_count, block_size, LANES), jnp.float32),
            pltpu.VMEM((chan_count, 1, width), jnp.float32),
            pltpu.VMEM((slots, block_size, 2 * width), jnp.bfloat16),
            pltpu.SemaphoreType.DMA((chan_count, count + len(chosen) + 1)),
            pltpu.SemaphoreType.DMA,
            pltpu.SemaphoreType.DMA((slots, 2)),
        ],
        input_output_aliases=aliases,
        compiler_params=pltpu.CompilerParams(vmem_limit_bytes=VMEM_LIMIT),
        cost_estimate=pl.CostEstimate(
            flops=4 * chan_count * block_size * width * depth,
            bytes_accessed=4 * chan_count * block_size * (width + depth),
            transcendentals=0,
        ),
    )(places, *operands)


def per_device(voltages, auto_prev, station_order):
    rows, cols = lax.axis_size("row"), lax.axis_size("col")
    row, col = lax.axis_index("row"), lax.axis_index("col")
    height, all_channels, parts, samples = voltages.shape
    chan_count = all_channels // rows
    block_size = height * rows
    offsets = cols // 2 + 1

    def partner_row(turn, parity):
        even, odd = rows_distance(turn, 0, rows), rows_distance(turn, 1, rows)
        return (row ^ jnp.where(parity == 1, odd, even)).astype(jnp.int32)

    autos = [auto_prev]
    for distance in range(2, cols, 2):
        autos.append(swap_with(auto_prev, "col", distance))
    autos = jnp.concatenate(autos, axis=1)
    autos = jnp.concatenate([autos, swap_with(autos, "col", 1)], axis=1)
    own = []
    for turn in range(rows):
        own.append(piece_of(voltages, partner_row(turn, col % 2)[None], chan_count))
        if turn > 0:
            own[turn] = traded(own[turn], turn)

    places_of = [[partner_row(turn, parity) for turn in range(rows)] for parity in (col % 2, 1 - col % 2)]

    split = height % LANES == 0
    if not split:
        stacked = jnp.take(jnp.stack(own, axis=1), jnp.argsort(jnp.stack(places_of[0])), axis=1)
        own = [stacked.reshape(chan_count, block_size, parts * samples)]
    partners = [own]
    for _ in range(1, offsets):
        partners.append([])
        for piece in partners[-2]:
            partners[-1].append(from_behind(piece, "col"))

    first = (col - (offsets - 1)) % cols * block_size
    order = jnp.concatenate([station_order, station_order])
    order = lax.dynamic_slice_in_dim(order, first, offsets * block_size, 0)
    distance = (order // block_size) ^ col
    slot = distance // 2 + distance % 2 * (cols // 2)
    chosen = jnp.take(autos, slot * block_size + order % block_size, axis=1, mode="clip")
    inverse = 1.0 / jnp.sqrt(chosen)
    row_scale = inverse[:, (offsets - 1) * block_size :] * (1.0 / samples)
    row_scale = jnp.broadcast_to(row_scale[:, :, None], (chan_count, block_size, LANES))
    column_scale = inverse[:, None, :]

    shape = (chan_count, offsets, block_size, 2 * block_size)
    count = len(own)
    if split:
        places = [jnp.stack(places_of[0] + partner) for partner in places_of]
    else:
        places = [jnp.zeros((2,), jnp.int32)] * 2
    every, last = list(range(count)), offsets - 1
    tiles = [(offset, every) for offset in range(last)]
    tiles += [(last, [piece]) for piece in every]
    if count > 2:
        tiles = tiles[: last - 1] + tiles[last : last + 2] + [tiles[last - 1]] + tiles[last + 2 :]
    out = None
    for offset, pieces in tiles:
        out = tile_call(
            out,
            shape,
            places[offset % 2],
            own,
            partners[offset],
            row_scale,
            column_scale,
            offset,
            pieces,
        )
    return out


def solution(mesh):
    return jax.shard_map(
        per_device,
        mesh=mesh,
        in_specs=(P(("col", "row"), None, None, None), P("row", "col"), P()),
        out_specs=P("row", None, "col", None),
        check_vma=False,
    )
```

```python
import jax
import jax.numpy as jnp
from jax import lax
from jax.experimental import pallas as pl
from jax.experimental.pallas import tpu as pltpu
from jax.sharding import PartitionSpec as P


LANES = 128
VMEM_LIMIT = 255 * 256 * 1024


def swap_with(value, axis, distance):
    count = lax.axis_size(axis)
    return lax.ppermute(value, axis, [(i, i ^ distance) for i in range(count)])


def from_behind(value, axis):
    count = lax.axis_size(axis)
    return lax.ppermute(value, axis, [(i, (i + 1) % count) for i in range(count)])


def rows_distance(turn, parity, rows):
    if parity == 1 and turn in (1, 2) and rows > 2:
        return 3 - turn
    return turn


def traded(value, turn):
    rows, cols = lax.axis_size("row"), lax.axis_size("col")
    pairs = []
    for row in range(rows):
        for col in range(cols):
            other = row ^ rows_distance(turn, col % 2, rows)
            pairs.append((row * cols + col, other * cols + col))
    return lax.ppermute(value, ("row", "col"), pairs)


def gather_piece(group_ref, voltages_ref, out_ref):
    stations, chan_count, parts, samples = voltages_ref.shape
    for chan in range(chan_count):
        out_ref[chan] = voltages_ref[:, chan, :, :].reshape(stations, parts * samples)


def piece_of(voltages, group, chan_count):
    stations, _, parts, samples = voltages.shape
    steps = 2 if stations % 32 == 0 else 1
    some = stations // steps
    return pl.pallas_call(
        gather_piece,
        grid_spec=pltpu.PrefetchScalarGridSpec(
            num_scalar_prefetch=1,
            grid=(steps,),
            in_specs=[
                pl.BlockSpec((some, chan_count, parts, samples), lambda i, at: (i, at[0], 0, 0))
            ],
            out_specs=pl.BlockSpec((chan_count, some, parts * samples), lambda i, at: (0, i, 0)),
        ),
        out_shape=jax.ShapeDtypeStruct((chan_count, stations, parts * samples), voltages.dtype),
    )(group, voltages)


def turned_of(rows):
    half = rows.shape[-1] // 2
    return jnp.concatenate([-rows[:, half:], rows[:, :half]], axis=-1)


def gram_of(left, right):
    return lax.dot_general(
        left, right, (((1,), (1,)), ((), ())), preferred_element_type=jnp.float32
    )


def tiles_kernel(count, chosen, offset, column_start, base, slots, places_ref, *refs):
    own, partner = refs[:count], refs[count : count + len(chosen)]
    row_scale_ref, column_scale_ref = refs[count + len(chosen) : count + len(chosen) + 2]
    out_ref, left_ref, right_ref, rows_ref, columns_ref, stage_ref, loaded, read, sent = refs[-9:]
    chan_count, height, _ = partner[0].shape
    block_size = height * count
    whole = len(chosen) == count
    width = height * len(chosen)
    first_column = column_start
    if not whole:
        first_column = pl.multiple_of(column_start + places_ref[count + chosen[0]] * height, LANES)

    def loads(chan):
        result = []
        for index, ref in enumerate([*own, *partner]):
            to_ref = left_ref if index < count else right_ref
            top = 0
            if index < count or whole:
                top = pl.multiple_of(places_ref[index] * height, height)
            source = ref.at[base + chan] if index < count else ref.at[chan]
            result.append((source, to_ref.at[chan, pl.ds(top, height)]))
        result.append((row_scale_ref.at[base + chan], rows_ref.at[chan]))
        return [
            pltpu.make_async_copy(source, target, loaded.at[chan, index])
            for index, (source, target) in enumerate(result)
        ]

    def sends(chan):
        slot = chan % slots
        if whole:
            return [pltpu.make_async_copy(stage_ref.at[slot], out_ref.at[base + chan, offset], sent.at[slot, 0])]
        result = []
        for part in range(2):
            column = part * block_size + places_ref[count + chosen[0]] * height
            column = pl.multiple_of(column, LANES)
            result.append(
                pltpu.make_async_copy(
                    stage_ref.at[slot, :, pl.ds(part * height, height)],
                    out_ref.at[base + chan, offset, :, pl.ds(column, height)],
                    sent.at[slot, part],
                )
            )
        return result

    columns_load = pltpu.make_async_copy(
        column_scale_ref.at[pl.ds(base, chan_count), :, pl.ds(first_column, width)], columns_ref, read
    )
    columns_load.start()

    def start_loads(chan, carry):
        for copy in loads(chan):
            copy.start()
        return carry

    lax.fori_loop(0, chan_count, start_loads, 0)
    columns_load.wait()

    def one_channel(chan, carry):
        slot = chan % slots
        for copy in loads(chan):
            copy.wait()
        if slots < chan_count:

            @pl.when(chan >= slots)
            def _():
                for copy in sends(chan - slots):
                    copy.wait()

        left = left_ref[chan]
        row_scale = rows_ref[chan]
        for lane in range(0, width, LANES):
            right = right_ref[chan, lane : lane + LANES, :]
            gram = gram_of(left, jnp.concatenate([right, turned_of(right)], axis=0))
            scale = columns_ref[chan, :, lane : lane + LANES]
            for part in range(2):
                tile = gram[:, part * LANES : (part + 1) * LANES] * row_scale * scale
                column = part * width + lane
                stage_ref[slot, :, column : column + LANES] = tile.astype(stage_ref.dtype)
        for copy in sends(chan):
            copy.start()
        return carry

    lax.fori_loop(0, chan_count, one_channel, 0)

    def drain(chan, carry):
        for copy in sends(chan):
            copy.wait()
        return carry

    lax.fori_loop(chan_count - slots, chan_count, drain, 0)


def tile_call(out, shape, places, own, partner, row_scale, column_scale, offset, chosen, base=0):
    _, offsets, block_size, _ = shape
    count, (chan_count, height, depth) = len(own), partner[0].shape
    slots = 2 if len(chosen) == count else chan_count
    width = height * len(chosen)
    operands = [*own, *partner, row_scale, column_scale]
    aliases = {}
    if out is not None:
        aliases = {1 + len(operands): 0}
        operands.append(out)
    in_specs = [pl.BlockSpec(memory_space=pltpu.SMEM)]
    in_specs += [pl.BlockSpec(memory_space=pl.ANY)] * len(operands)
    column_start = (offsets - 1 - offset) * block_size

    def body(*refs):
        tiles_kernel(count, chosen, offset, column_start, base, slots, *refs)

    return pl.pallas_call(
        body,
        in_specs=in_specs,
        out_specs=pl.BlockSpec(memory_space=pl.ANY),
        out_shape=jax.ShapeDtypeStruct(shape, jnp.bfloat16),
        scratch_shapes=[
            pltpu.VMEM((chan_count, block_size, depth), jnp.bfloat16),
            pltpu.VMEM((chan_count, width, depth), jnp.bfloat16),
            pltpu.VMEM((chan_count, block_size, LANES), jnp.float32),
            pltpu.VMEM((chan_count, 1, width), jnp.float32),
            pltpu.VMEM((slots, block_size, 2 * width), jnp.bfloat16),
            pltpu.SemaphoreType.DMA((chan_count, count + len(chosen) + 1)),
            pltpu.SemaphoreType.DMA,
            pltpu.SemaphoreType.DMA((slots, 2)),
        ],
        input_output_aliases=aliases,
        compiler_params=pltpu.CompilerParams(vmem_limit_bytes=VMEM_LIMIT),
        cost_estimate=pl.CostEstimate(
            flops=4 * chan_count * block_size * width * depth,
            bytes_accessed=4 * chan_count * block_size * (width + depth),
            transcendentals=0,
        ),
    )(places, *operands)


def per_device(voltages, auto_prev, station_order):
    rows, cols = lax.axis_size("row"), lax.axis_size("col")
    row, col = lax.axis_index("row"), lax.axis_index("col")
    height, all_channels, parts, samples = voltages.shape
    chan_count = all_channels // rows
    block_size = height * rows
    offsets = cols // 2 + 1

    def partner_row(turn, parity):
        even, odd = rows_distance(turn, 0, rows), rows_distance(turn, 1, rows)
        return (row ^ jnp.where(parity == 1, odd, even)).astype(jnp.int32)

    autos = [auto_prev]
    for distance in range(2, cols, 2):
        autos.append(swap_with(auto_prev, "col", distance))
    autos = jnp.concatenate(autos, axis=1)
    autos = jnp.concatenate([autos, swap_with(autos, "col", 1)], axis=1)
    own = []
    for turn in range(rows):
        own.append(piece_of(voltages, partner_row(turn, col % 2)[None], chan_count))
        if turn > 0:
            own[turn] = traded(own[turn], turn)

    places_of = [[partner_row(turn, parity) for turn in range(rows)] for parity in (col % 2, 1 - col % 2)]

    split = height % LANES == 0
    if not split:
        stacked = jnp.take(jnp.stack(own, axis=1), jnp.argsort(jnp.stack(places_of[0])), axis=1)
        own = [stacked.reshape(chan_count, block_size, parts * samples)]
    partners = [own]
    for offset in range(1, offsets):
        partners.append([])
        for index, piece in enumerate(partners[-2]):
            if split and offset == offsets - 1 and index == len(own) - 1:
                half = chan_count // 2
                lower, upper = piece[:half], piece[half:]
                lower = from_behind(lower, "col")
                upper = from_behind(upper, "col")
                partners[-1].append([lower, upper])
                continue
            partners[-1].append(from_behind(piece, "col"))

    first = (col - (offsets - 1)) % cols * block_size
    order = jnp.concatenate([station_order, station_order])
    order = lax.dynamic_slice_in_dim(order, first, offsets * block_size, 0)
    distance = (order // block_size) ^ col
    slot = distance // 2 + distance % 2 * (cols // 2)
    chosen = jnp.take(autos, slot * block_size + order % block_size, axis=1, mode="clip")
    inverse = 1.0 / jnp.sqrt(chosen)
    row_scale = inverse[:, (offsets - 1) * block_size :] * (1.0 / samples)
    row_scale = jnp.broadcast_to(row_scale[:, :, None], (chan_count, block_size, LANES))
    column_scale = inverse[:, None, :]

    shape = (chan_count, offsets, block_size, 2 * block_size)
    count = len(own)
    if split:
        places = [jnp.stack(places_of[0] + partner) for partner in places_of]
    else:
        places = [jnp.zeros((2,), jnp.int32)] * 2
    every, last = list(range(count)), offsets - 1
    tiles = [(offset, every) for offset in range(last)]
    tiles += [(last, [piece]) for piece in every]
    if count > 2:
        tiles = tiles[: last - 1] + tiles[last : last + 2] + [tiles[last - 1]] + tiles[last + 2 :]
    out = None
    for offset, pieces in tiles:
        base = 0
        partner = [partners[offset][piece] for piece in pieces]
        for part in partner[0] if isinstance(partner[0], list) else [None]:
            out = tile_call(
                out,
                shape,
                places[offset % 2],
                own,
                partner if part is None else [part],
                row_scale,
                column_scale,
                offset,
                pieces,
                base,
            )
            base += 0 if part is None else part.shape[0]
    return out


def solution(mesh):
    return jax.shard_map(
        per_device,
        mesh=mesh,
        in_specs=(P(("col", "row"), None, None, None), P("row", "col"), P()),
        out_specs=P("row", None, "col", None),
        check_vma=False,
    )
```
